32 devices in a mesh: dp: 8 (over z, y), tensor: 4 (over x, core).
Axes of the slice: x: 2, y: 2, z: 4, core: 2. Of those that a mesh axis runs over, the one named last changes fastest.
Arguments:
- attn_out: bfloat16 [2048, 4096], P('dp', 'tensor'), may hold values from -6 to 6
- w_blocks: bfloat16 [4096, 8192], P('tensor', 'dp'), may hold values from -0.09375 to 0.09375
- w_scales: float32 [32, 8192], P('tensor', 'dp'), may hold values from 0.5 to 2
- residual: bfloat16 [2048, 8192], P('dp')
- gain: float32 [8192], P('tensor'), may hold values from 0.5 to 1.5
Outputs:
- hidden: bfloat16 [2048, 8192], P('dp', 'tensor')
- normed: bfloat16 [2048, 8192], P('dp', 'tensor')
The draws below stay inside these ranges and needn't reach their ends.
All inputs are finite; a program needn't handle non-finite values.
Results may differ from the reference program's by a relative error of at most 0.014.
Values may be sent and summed in bfloat16 or wider, within the bound.
A program may use at most 128 MiB of HBM per device.

```python
import math
import jax
import jax.numpy as jnp
from jax import lax

D = 8192
BLOCK = 128
HD = 4096
TOKENS = 2048


def draw_residual(key, part):
    first = jax.random.fold_in(jax.random.fold_in(key, 17), 0)
    base = jnp.clip(jax.random.normal(first, (TOKENS, D), jnp.float32), -6.0, 6.0)
    ramp = 0.6 * jnp.exp(math.log(3.0) * jnp.arange(D, dtype=jnp.float32) / D)
    return (base * ramp[None, :]).astype(jnp.bfloat16)


def shard_levels(rng, extent, shards, smallest, high):
    level, own = 1.0, jax.random.fold_in(rng, 6)
    for dim, parts in shards:
        heights = jnp.exp(jax.random.uniform(jax.random.fold_in(own, dim), (parts,), jnp.float32, smallest / len(shards), high / len(shards)))
        level = level * jnp.repeat(heights, extent[dim] // parts).reshape([-1 if axis == dim else 1 for axis in range(len(extent))])
    return level


def bell_draw(own_key, shape, scale, most, cuts=(), held_as=jnp.bfloat16):
    values = jax.random.normal(own_key, shape, jnp.float32) * scale
    if len(cuts) > 0:
        values = shard_levels(own_key, shape, cuts, -0.22, 0.18) * values
    return jnp.clip(values, min=-most, max=most).astype(held_as)


def setup_inputs(seed: int = 0) -> dict:
    key_list = jax.random.split(jax.random.key(seed), 6)
    attn_out = bell_draw(key_list[0], (TOKENS, HD), 1.0, 6.0, ((0, 8), (1, 4)))
    w_blocks = bell_draw(key_list[1], (HD, D), HD ** -0.5, 0.09375, ((0, 4), (1, 8)))
    w_scales = jnp.clip(jnp.exp(math.log(2.0) - 1.3862944 * jax.random.uniform(key_list[2], (HD // BLOCK, D), jnp.float32) ** shard_levels(key_list[2], (HD // BLOCK, D), ((0, 4), (1, 8)), -0.2, 0.2)), 0.5, 2.0)
    residual = draw_residual(jax.random.fold_in(key_list[5], 71), 0)
    gain = jnp.clip(1.0 + 0.1 * jax.random.normal(key_list[4], (D,), jnp.float32), 0.5, 1.5)
    return {"attn_out": attn_out, "w_blocks": w_blocks, "w_scales": w_scales, "residual": residual, "gain": gain}


def dequantize(blocks, scales):
    spread = jnp.repeat(scales, BLOCK, axis=0)
    return (blocks.astype(jnp.float32) * spread).astype(jnp.bfloat16)

def reference(attn_out, w_blocks, w_scales, residual, gain):
    weights = dequantize(w_blocks, w_scales)
    attn_sum = jnp.dot(attn_out, weights, preferred_element_type=jnp.float32)
    hidden = (residual.astype(jnp.float32) + attn_sum).astype(jnp.bfloat16)
    wide = hidden.astype(jnp.float32)
    mean_square = lax.optimization_barrier(jnp.sum(wide * wide, axis=1, keepdims=True)) / D
    normed = (wide * gain[None, :] * jax.lax.rsqrt(mean_square + 1e-05)).astype(jnp.bfloat16)
    return (hidden, normed)
```

```python
import functools

import jax
import jax.numpy as jnp
from jax import lax
from jax.experimental import pallas as pl
from jax.experimental.pallas import tpu as pltpu
from jax.sharding import PartitionSpec as P

MESH = pl.DeviceIdType.MESH
WIDTH = 256
LANES = 128


def plan(dp, groups, cols):
    inner = dp // groups
    width = min(WIDTH, cols)
    own = cols // width
    peers = (inner - 1) * own
    wave_of_seg = [0] * own + [1 + p * groups // peers for p in range(peers)]
    waves = [[] for _ in range(groups + 1)]
    for j in range(groups):
        for s, at in enumerate(wave_of_seg):
            waves[max(j, at)].append((j, s))
    return inner, width, own, wave_of_seg, waves


def kernel(
    dp, groups,
    a_ref, w_ref, sc_ref, res_hbm, gain_ref,
    hidden_ref, normed_ref,
    a_buf, w_buf, sc_buf, wd, res, part,
    snd1, rcv1, keep2, snd2, rcv2, snd3, zin, hs, acc, scl_snd, scl,
    res_sem, a_send, a_recv, w_send, w_recv, sc_send, sc_recv,
    s1, r1, s2, r2, s3, r3, s4, r4, s5, r5,
):
    rows, depth = a_ref.shape
    cols = w_ref.shape[1]
    my_cols = hidden_ref.shape[1]
    blocks = sc_ref.shape[0]
    per_block = depth // blocks
    half, quarter = rows // 2, rows // 4
    inner, width, own, wave_of_seg, waves = plan(dp, groups, cols)
    segs = len(wave_of_seg)

    d = lax.axis_index("dp")
    t = lax.axis_index("tensor")
    z, i = d // inner, d % inner
    core, x = t % 2, t // 2
    core_peer = t + 1 - 2 * core
    x_peer = (t + 2) % 4

    def line(o):
        return {"dp": o * inner + i, "tensor": t}

    def row(other):
        return {"dp": d, "tensor": other}

    def pair(other):
        return {"dp": z * inner + other, "tensor": t}

    def step_block(j):
        if j == 0:
            return z
        if j == 1:
            return z + 1 - 2 * (z % 2)
        if j == 2:
            return z + 2 - 4 * (z // 2)
        return 3 - z

    def row_offset(who):
        return pl.multiple_of((who % 2) * half + (who // 2) * quarter, quarter)

    def seg_col(s):
        return pl.multiple_of(((i + s // own) % inner) * cols + (s % own) * width, width)

    def remote(src, dst, send, recv, to):
        return pltpu.make_async_remote_copy(
            src_ref=src, dst_ref=dst, send_sem=send, recv_sem=recv,
            device_id=to, device_id_type=MESH,
        )

    mine = row_offset(t)
    res_copy = pltpu.make_async_copy(res_hbm.at[pl.ds(mine, quarter), :], res, res_sem)
    res_copy.start()

    barrier = pltpu.get_barrier_semaphore()
    for r in range(1, inner):
        pl.semaphore_signal(barrier, inc=1, device_id=pair((i + r) % inner), device_id_type=MESH)
    for r in range(1, groups):
        pl.semaphore_signal(barrier, inc=1, device_id=line((z + r) % groups), device_id_type=MESH)
    for r in range(1, 4):
        pl.semaphore_signal(barrier, inc=1, device_id=row((t + r) % 4), device_id_type=MESH)
    pl.semaphore_wait(barrier, inner - 1 + groups - 1 + 3)

    def a_copy(src, block, send, to):
        return remote(src, a_buf.at[block], a_send.at[send], a_recv.at[block], line(to))

    @pl.when(z < groups - 1)
    def _():
        a_copy(a_ref, z, z, z + 1).start()

    @pl.when(z > 0)
    def _():
        a_copy(a_ref, z, groups, z - 1).start()

    def sc_copy(r):
        return remote(sc_ref, sc_buf.at[r - 1], sc_send.at[r - 1], sc_recv.at[r - 1], pair((i + inner - r) % inner))

    def w_copy(r, c):
        k = (r - 1) * own + c
        return remote(
            w_ref.at[:, pl.ds(c * width, width)], w_buf.at[k], w_send.at[k], w_recv.at[k],
            pair((i + inner - r) % inner),
        )

    for r in range(1, inner):
        sc_copy(r).start()
    for r in range(1, inner):
        for c in range(own):
            w_copy(r, c).start()

    def dequantize(s):
        c = s % own
        for b in range(blocks):
            lines = pl.ds(b * per_block, per_block)
            if s < own:
                raw = w_ref[lines, pl.ds(c * width, width)]
                scale = sc_ref[pl.ds(b, 1), pl.ds(c * width, width)]
            else:
                raw = w_buf[s - own, lines, :]
                scale = sc_buf[s // own - 1, pl.ds(b, 1), pl.ds(c * width, width)]
            wd[s, lines, :] = (raw.astype(jnp.float32) * scale).astype(jnp.bfloat16)

    def forward(k):
        @pl.when(z >= k)
        def _():
            b = z - k
            a_copy(a_ref, b, b, z).wait_recv()

            @pl.when(z < groups - 1)
            def _():
                a_copy(a_buf.at[b], b, b, z + 1).start()

        @pl.when(z + k <= groups - 1)
        def _():
            b = z + k
            a_copy(a_ref, b, b, z).wait_recv()

            @pl.when(z > 0)
            def _():
                a_copy(a_buf.at[b], b, b, z - 1).start()

    def copy1(u):
        return remote(snd1.at[u], rcv1.at[u], s1.at[u], r1.at[u], row(core_peer))

    def copy2(u):
        return remote(snd2.at[u], rcv2.at[u], s2.at[u], r2.at[u], row(x_peer))

    def copy3(u, j):
        return remote(snd3.at[u], zin.at[u], s3.at[u], r3.at[u], line(step_block(j)))

    def copy4(u, j, s):
        return remote(
            hs.at[u], hidden_ref.at[pl.ds(mine, quarter), pl.ds(seg_col(s), width)],
            s4.at[u], r4.at[t * segs + s], row(step_block(j)),
        )

    keep_rows = pl.multiple_of(core * half, half)
    send_rows = pl.multiple_of((1 - core) * half, half)

    def stage1(u, j, s):
        a = a_ref[...] if j == 0 else a_buf[step_block(j)]
        part[u % 2] = jnp.dot(a, wd[s], preferred_element_type=jnp.float32)
        snd1[u] = part[u % 2, pl.ds(send_rows, half), :].astype(jnp.bfloat16)
        copy1(u).start()

    def stage2(u):
        copy1(u).wait_recv()
        near = pl.multiple_of(x * quarter, quarter)
        far = pl.multiple_of((1 - x) * quarter, quarter)
        snd2[u] = (
            part[u % 2, pl.ds(pl.multiple_of(keep_rows + far, quarter), quarter), :]
            + rcv1[u, pl.ds(far, quarter), :].astype(jnp.float32)
        ).astype(jnp.bfloat16)
        copy2(u).start()
        keep2[u] = (
            part[u % 2, pl.ds(pl.multiple_of(keep_rows + near, quarter), quarter), :]
            + rcv1[u, pl.ds(near, quarter), :].astype(jnp.float32)
        )

    def stage3(u, j):
        copy2(u).wait_recv()
        total = (keep2[u] + rcv2[u].astype(jnp.float32)).astype(jnp.bfloat16)
        if j == 0:
            zin[u] = total
        else:
            snd3[u] = total
            copy3(u, j).start()

    def stage4(u, j, s):
        if j > 0:
            copy3(u, j).wait_recv()
        source = step_block(j)
        at = pl.multiple_of(source * my_cols + seg_col(s), width)
        h = (zin[u].astype(jnp.float32) + res[:, pl.ds(at, width)].astype(jnp.float32)).astype(jnp.bfloat16)
        hs[u] = h

        @pl.when(source != t)
        def _():
            copy4(u, j, s).start()

        @pl.when(source == t)
        def _():
            hidden_ref[pl.ds(mine, quarter), pl.ds(seg_col(s), width)] = hs[u]

        wide = h.astype(jnp.float32)
        square = wide * wide
        total = acc[...]
        for k in range(width // LANES):
            total = total + square[:, k * LANES:(k + 1) * LANES]
        acc[...] = total

    acc[...] = jnp.zeros_like(acc)
    number = 0
    late = []
    units = []
    for w, wave in enumerate(waves):
        if 1 <= w < groups:
            forward(w)
        for s in range(segs):
            if wave_of_seg[s] == w:
                if s >= own:
                    r, c = s // own, s % own
                    if c == 0:
                        sc_copy(r).wait_recv()
                    w_copy(r, c).wait_recv()
                dequantize(s)
        now = [(number + k, j, s) for k, (j, s) in enumerate(wave)]
        number += len(wave)
        for k, (u, j, s) in enumerate(now):
            stage1(u, j, s)
            if k > 0:
                stage2(now[k - 1][0])
        if now:
            stage2(now[-1][0])
        if w == 1:
            res_copy.wait()
        for u, j, s in late:
            stage4(u, j, s)
        for u, j, s in now:
            stage3(u, j)
        late = now
        units += now
    for u, j, s in late:
        stage4(u, j, s)

    mean_square = jnp.sum(acc[...], axis=1, keepdims=True) / (my_cols * groups)
    scl_snd[...] = jnp.broadcast_to(lax.rsqrt(mean_square + 1e-05), scl_snd.shape)
    scl[pl.ds(mine, quarter), :] = scl_snd[...]

    def copy5(r):
        return remote(
            scl_snd, scl.at[pl.ds(mine, quarter), :], s5.at[r - 1], r5.at[t], row((t + r) % 4)
        )

    for r in range(1, 4):
        copy5(r).start()

    def normalize(who):
        at = pl.ds(row_offset(who), quarter)
        scale = scl[at, :]
        for k in range(my_cols // LANES):
            lanes = pl.ds(k * LANES, LANES)
            normed_ref[at, lanes] = (
                hidden_ref[at, lanes].astype(jnp.float32) * gain_ref[:, lanes] * scale
            ).astype(jnp.bfloat16)

    normalize(t)
    for r in range(1, 4):
        who = (t + r) % 4
        at = pl.ds(row_offset(who), quarter)
        for s in range(segs):
            piece = hidden_ref.at[at, pl.ds(seg_col(s), width)]
            remote(hs.at[0], piece, s4.at[0], r4.at[who * segs + s], row(who)).wait_recv()
        remote(scl_snd, scl.at[at, :], s5.at[0], r5.at[who], row(who)).wait_recv()
        normalize(who)

    @pl.when(z < groups - 1)
    def _():
        a_copy(a_ref, z, z, z + 1).wait_send()

    @pl.when(z > 0)
    def _():
        a_copy(a_ref, z, groups, z - 1).wait_send()

    for k in range(1, groups):
        @pl.when((z >= k) & (z < groups - 1))
        def _():
            a_copy(a_ref, z - k, z - k, z + 1).wait_send()

        @pl.when((z + k <= groups - 1) & (z > 0))
        def _():
            a_copy(a_ref, z + k, z + k, z - 1).wait_send()

    for r in range(1, inner):
        sc_copy(r).wait_send()
        for c in range(own):
            w_copy(r, c).wait_send()
    for u, j, s in units:
        copy1(u).wait_send()
        copy2(u).wait_send()
        if j > 0:
            copy3(u, j).wait_send()

        @pl.when(step_block(j) != t)
        def _():
            copy4(u, j, s).wait_send()
    for r in range(1, 4):
        copy5(r).wait_send()


def solution(mesh):
    dp, groups = mesh.shape["dp"], mesh.shape["tensor"]

    def on_device(attn_out, w_blocks, w_scales, residual, gain):
        rows, depth = attn_out.shape
        cols = w_blocks.shape[1]
        my_cols = gain.shape[0]
        inner, width, own, wave_of_seg, waves = plan(dp, groups, cols)
        segs = len(wave_of_seg)
        n = segs * groups
        peers = segs - own
        half, quarter = rows // 2, rows // 4
        bf16, f32 = jnp.bfloat16, jnp.float32
        vmem = pl.BlockSpec(memory_space=pltpu.VMEM)
        dma = pltpu.SemaphoreType.DMA
        out = jax.ShapeDtypeStruct((rows, my_cols), bf16)
        return tuple(pl.pallas_call(
            functools.partial(kernel, dp, groups),
            out_shape=(out, out),
            in_specs=[vmem, vmem, vmem, pl.BlockSpec(memory_space=pl.ANY), vmem],
            out_specs=(vmem, vmem),
            scratch_shapes=[
                pltpu.VMEM((groups, rows, depth), bf16),
                pltpu.VMEM((peers, depth, width), bf16),
                pltpu.VMEM((inner - 1,) + w_scales.shape, f32),
                pltpu.VMEM((segs, depth, width), bf16),
                pltpu.VMEM((quarter, residual.shape[1]), bf16),
                pltpu.VMEM((2, rows, width), f32),
                pltpu.VMEM((n, half, width), bf16),
                pltpu.VMEM((n, half, width), bf16),
                pltpu.VMEM((n, quarter, width), f32),
                pltpu.VMEM((n, quarter, width), bf16),
                pltpu.VMEM((n, quarter, width), bf16),
                pltpu.VMEM((n, quarter, width), bf16),
                pltpu.VMEM((n, quarter, width), bf16),
                pltpu.VMEM((n, quarter, width), bf16),
                pltpu.VMEM((quarter, LANES), f32),
                pltpu.VMEM((quarter, LANES), f32),
                pltpu.VMEM((rows, LANES), f32),
                dma, dma((groups + 1,)), dma((groups,)), dma((peers,)), dma((peers,)),
                dma((inner - 1,)), dma((inner - 1,)),
                dma((n,)), dma((n,)), dma((n,)), dma((n,)), dma((n,)), dma((n,)),
                dma((n,)), dma((groups * segs,)), dma((3,)), dma((groups,)),
            ],
            compiler_params=pltpu.CompilerParams(
                collective_id=0, has_side_effects=True, vmem_limit_bytes=60 * 1024 * 1024,
            ),
        )(attn_out, w_blocks, w_scales, residual, gain.reshape(1, my_cols)))

    return jax.shard_map(
        on_device,
        mesh=mesh,
        in_specs=(
            P("dp", "tensor"),
            P("tensor", "dp"),
            P("tensor", "dp"),
            P("dp", None),
            P("tensor"),
        ),
        out_specs=(P("dp", "tensor"), P("dp", "tensor")),
        check_vma=False,
    )
```

```python
import functools

import jax
import jax.numpy as jnp
from jax import lax
from jax.experimental import pallas as pl
from jax.experimental.pallas import tpu as pltpu
from jax.sharding import PartitionSpec as P

MESH = pl.DeviceIdType.MESH
WIDTH = 256
LANES = 128


def plan(dp, groups, cols):
    inner = dp // groups
    width = min(WIDTH, cols)
    own = cols // width
    peers = (inner - 1) * own
    wave_of_seg = [0] * own + [1 + p * groups // peers for p in range(peers)]
    waves = [[] for _ in range(groups + 1)]
    for j in range(groups):
        for s, at in enumerate(wave_of_seg):
            waves[max(j, at)].append((j, s))
    return inner, width, own, wave_of_seg, waves


def kernel(
    dp, groups,
    a_ref, w_ref, sc_ref, res_hbm,
    hidden_ref, scl,
    a_buf, w_buf, sc_buf, wd, res, part,
    snd1, rcv1, keep2, snd2, rcv2, snd3, zin, hs, acc, scl_snd,
    res_sem, a_send, a_recv, w_send, w_recv, sc_send, sc_recv,
    s1, r1, s2, r2, s3, r3, s4, r4, s5, r5,
):
    rows, depth = a_ref.shape
    cols = w_ref.shape[1]
    my_cols = hidden_ref.shape[1]
    blocks = sc_ref.shape[0]
    per_block = depth // blocks
    half, quarter = rows // 2, rows // 4
    inner, width, own, wave_of_seg, waves = plan(dp, groups, cols)
    segs = len(wave_of_seg)

    d = lax.axis_index("dp")
    t = lax.axis_index("tensor")
    z, i = d // inner, d % inner
    core, x = t % 2, t // 2
    core_peer = t + 1 - 2 * core
    x_peer = (t + 2) % 4

    def line(o):
        return {"dp": o * inner + i, "tensor": t}

    def row(other):
        return {"dp": d, "tensor": other}

    def pair(other):
        return {"dp": z * inner + other, "tensor": t}

    def step_block(j):
        if j == 0:
            return z
        if j == 1:
            return z + 1 - 2 * (z % 2)
        if j == 2:
            return z + 2 - 4 * (z // 2)
        return 3 - z

    def row_offset(who):
        return pl.multiple_of((who % 2) * half + (who // 2) * quarter, quarter)

    def seg_col(s):
        return pl.multiple_of(((i + s // own) % inner) * cols + (s % own) * width, width)

    def remote(src, dst, send, recv, to):
        return pltpu.make_async_remote_copy(
            src_ref=src, dst_ref=dst, send_sem=send, recv_sem=recv,
            device_id=to, device_id_type=MESH,
        )

    mine = row_offset(t)
    res_copy = pltpu.make_async_copy(res_hbm.at[pl.ds(mine, quarter), :], res, res_sem)
    res_copy.start()

    barrier = pltpu.get_barrier_semaphore()
    for r in range(1, inner):
        pl.semaphore_signal(barrier, inc=1, device_id=pair((i + r) % inner), device_id_type=MESH)
    for r in range(1, groups):
        pl.semaphore_signal(barrier, inc=1, device_id=line((z + r) % groups), device_id_type=MESH)
    for r in range(1, 4):
        pl.semaphore_signal(barrier, inc=1, device_id=row((t + r) % 4), device_id_type=MESH)
    pl.semaphore_wait(barrier, inner - 1 + groups - 1 + 3)

    def a_copy(src, block, send, to):
        return remote(src, a_buf.at[block], a_send.at[send], a_recv.at[block], line(to))

    @pl.when(z < groups - 1)
    def _():
        a_copy(a_ref, z, z, z + 1).start()

    @pl.when(z > 0)
    def _():
        a_copy(a_ref, z, groups, z - 1).start()

    def sc_copy(r):
        return remote(sc_ref, sc_buf.at[r - 1], sc_send.at[r - 1], sc_recv.at[r - 1], pair((i + inner - r) % inner))

    def w_copy(r, c):
        k = (r - 1) * own + c
        return remote(
            w_ref.at[:, pl.ds(c * width, width)], w_buf.at[k], w_send.at[k], w_recv.at[k],
            pair((i + inner - r) % inner),
        )

    for r in range(1, inner):
        sc_copy(r).start()
    for r in range(1, inner):
        for c in range(own):
            w_copy(r, c).start()

    def dequantize(s):
        c = s % own
        for b in range(blocks):
            lines = pl.ds(b * per_block, per_block)
            if s < own:
                raw = w_ref[lines, pl.ds(c * width, width)]
                scale = sc_ref[pl.ds(b, 1), pl.ds(c * width, width)]
            else:
                raw = w_buf[s - own, lines, :]
                scale = sc_buf[s // own - 1, pl.ds(b, 1), pl.ds(c * width, width)]
            wd[s, lines, :] = (raw.astype(jnp.float32) * scale).astype(jnp.bfloat16)

    def forward(k):
        @pl.when(z >= k)
        def _():
            b = z - k
            a_copy(a_ref, b, b, z).wait_recv()

            @pl.when(z < groups - 1)
            def _():
                a_copy(a_buf.at[b], b, b, z + 1).start()

        @pl.when(z + k <= groups - 1)
        def _():
            b = z + k
            a_copy(a_ref, b, b, z).wait_recv()

            @pl.when(z > 0)
            def _():
                a_copy(a_buf.at[b], b, b, z - 1).start()

    def copy1(u):
        return remote(snd1.at[u], rcv1.at[u], s1.at[u], r1.at[u], row(core_peer))

    def copy2(u):
        return remote(snd2.at[u], rcv2.at[u], s2.at[u], r2.at[u], row(x_peer))

    def copy3(u, j):
        return remote(snd3.at[u], zin.at[u], s3.at[u], r3.at[u], line(step_block(j)))

    def copy4(u, j, s):
        return remote(
            hs.at[u], hidden_ref.at[pl.ds(mine, quarter), pl.ds(seg_col(s), width)],
            s4.at[u], r4.at[t * segs + s], row(step_block(j)),
        )

    keep_rows = pl.multiple_of(core * half, half)
    send_rows = pl.multiple_of((1 - core) * half, half)

    def stage1(u, j, s):
        a = a_ref[...] if j == 0 else a_buf[step_block(j)]
        part[u % 2] = jnp.dot(a, wd[s], preferred_element_type=jnp.float32)
        snd1[u] = part[u % 2, pl.ds(send_rows, half), :].astype(jnp.bfloat16)
        copy1(u).start()

    def stage2(u):
        copy1(u).wait_recv()
        near = pl.multiple_of(x * quarter, quarter)
        far = pl.multiple_of((1 - x) * quarter, quarter)
        snd2[u] = (
            part[u % 2, pl.ds(pl.multiple_of(keep_rows + far, quarter), quarter), :]
            + rcv1[u, pl.ds(far, quarter), :].astype(jnp.float32)
        ).astype(jnp.bfloat16)
        copy2(u).start()
        keep2[u] = (
            part[u % 2, pl.ds(pl.multiple_of(keep_rows + near, quarter), quarter), :]
            + rcv1[u, pl.ds(near, quarter), :].astype(jnp.float32)
        )

    def stage3(u, j):
        copy2(u).wait_recv()
        total = (keep2[u] + rcv2[u].astype(jnp.float32)).astype(jnp.bfloat16)
        if j == 0:
            zin[u] = total
        else:
            snd3[u] = total
            copy3(u, j).start()

    def stage4(u, j, s):
        if j > 0:
            copy3(u, j).wait_recv()
        source = step_block(j)
        at = pl.multiple_of(source * my_cols + seg_col(s), width)
        h = (zin[u].astype(jnp.float32) + res[:, pl.ds(at, width)].astype(jnp.float32)).astype(jnp.bfloat16)
        hs[u] = h

        @pl.when(source != t)
        def _():
            copy4(u, j, s).start()

        @pl.when(source == t)
        def _():
            hidden_ref[pl.ds(mine, quarter), pl.ds(seg_col(s), width)] = hs[u]

        wide = h.astype(jnp.float32)
        square = wide * wide
        total = acc[...]
        for k in range(width // LANES):
            total = total + square[:, k * LANES:(k + 1) * LANES]
        acc[...] = total

    acc[...] = jnp.zeros_like(acc)
    number = 0
    late = []
    units = []
    for w, wave in enumerate(waves):
        if 1 <= w < groups:
            forward(w)
        for s in range(segs):
            if wave_of_seg[s] == w:
                if s >= own:
                    r, c = s // own, s % own
                    if c == 0:
                        sc_copy(r).wait_recv()
                    w_copy(r, c).wait_recv()
                dequantize(s)
        now = [(number + k, j, s) for k, (j, s) in enumerate(wave)]
        number += len(wave)
        for k, (u, j, s) in enumerate(now):
            stage1(u, j, s)
            if k > 0:
                stage2(now[k - 1][0])
        if now:
            stage2(now[-1][0])
        if w == 1:
            res_copy.wait()
        for u, j, s in late:
            stage4(u, j, s)
        for u, j, s in now:
            stage3(u, j)
        late = now
        units += now
    for u, j, s in late:
        stage4(u, j, s)

    mean_square = jnp.sum(acc[...], axis=1, keepdims=True) / (my_cols * groups)
    scl_snd[...] = jnp.broadcast_to(lax.rsqrt(mean_square + 1e-05), scl_snd.shape)
    scl[pl.ds(mine, quarter), :] = scl_snd[...]

    def copy5(r):
        return remote(
            scl_snd, scl.at[pl.ds(mine, quarter), :], s5.at[r - 1], r5.at[t], row((t + r) % 4)
        )

    for r in range(1, 4):
        copy5(r).start()

    for r in range(1, 4):
        who = (t + r) % 4
        at = pl.ds(row_offset(who), quarter)
        for s in range(segs):
            piece = hidden_ref.at[at, pl.ds(seg_col(s), width)]
            remote(hs.at[0], piece, s4.at[0], r4.at[who * segs + s], row(who)).wait_recv()
        remote(scl_snd, scl.at[at, :], s5.at[0], r5.at[who], row(who)).wait_recv()

    @pl.when(z < groups - 1)
    def _():
        a_copy(a_ref, z, z, z + 1).wait_send()

    @pl.when(z > 0)
    def _():
        a_copy(a_ref, z, groups, z - 1).wait_send()

    for k in range(1, groups):
        @pl.when((z >= k) & (z < groups - 1))
        def _():
            a_copy(a_ref, z - k, z - k, z + 1).wait_send()

        @pl.when((z + k <= groups - 1) & (z > 0))
        def _():
            a_copy(a_ref, z + k, z + k, z - 1).wait_send()

    for r in range(1, inner):
        sc_copy(r).wait_send()
        for c in range(own):
            w_copy(r, c).wait_send()
    for u, j, s in units:
        copy1(u).wait_send()
        copy2(u).wait_send()
        if j > 0:
            copy3(u, j).wait_send()

        @pl.when(step_block(j) != t)
        def _():
            copy4(u, j, s).wait_send()
    for r in range(1, 4):
        copy5(r).wait_send()


def solution(mesh):
    dp, groups = mesh.shape["dp"], mesh.shape["tensor"]

    def on_device(attn_out, w_blocks, w_scales, residual, gain):
        rows, depth = attn_out.shape
        cols = w_blocks.shape[1]
        my_cols = gain.shape[0]
        inner, width, own, wave_of_seg, waves = plan(dp, groups, cols)
        segs = len(wave_of_seg)
        n = segs * groups
        peers = segs - own
        half, quarter = rows // 2, rows // 4
        bf16, f32 = jnp.bfloat16, jnp.float32
        vmem = pl.BlockSpec(memory_space=pltpu.VMEM)
        dma = pltpu.SemaphoreType.DMA
        out = jax.ShapeDtypeStruct((rows, my_cols), bf16)
        hidden, scale = pl.pallas_call(
            functools.partial(kernel, dp, groups),
            out_shape=(out, jax.ShapeDtypeStruct((rows, LANES), f32)),
            in_specs=[vmem, vmem, vmem, pl.BlockSpec(memory_space=pl.ANY)],
            out_specs=(vmem, vmem),
            scratch_shapes=[
                pltpu.VMEM((groups, rows, depth), bf16),
                pltpu.VMEM((peers, depth, width), bf16),
                pltpu.VMEM((inner - 1,) + w_scales.shape, f32),
                pltpu.VMEM((segs, depth, width), bf16),
                pltpu.VMEM((quarter, residual.shape[1]), bf16),
                pltpu.VMEM((2, rows, width), f32),
                pltpu.VMEM((n, half, width), bf16),
                pltpu.VMEM((n, half, width), bf16),
                pltpu.VMEM((n, quarter, width), f32),
                pltpu.VMEM((n, quarter, width), bf16),
                pltpu.VMEM((n, quarter, width), bf16),
                pltpu.VMEM((n, quarter, width), bf16),
                pltpu.VMEM((n, quarter, width), bf16),
                pltpu.VMEM((n, quarter, width), bf16),
                pltpu.VMEM((quarter, LANES), f32),
                pltpu.VMEM((quarter, LANES), f32),
                dma, dma((groups + 1,)), dma((groups,)), dma((peers,)), dma((peers,)),
                dma((inner - 1,)), dma((inner - 1,)),
                dma((n,)), dma((n,)), dma((n,)), dma((n,)), dma((n,)), dma((n,)),
                dma((n,)), dma((groups * segs,)), dma((3,)), dma((groups,)),
            ],
            compiler_params=pltpu.CompilerParams(
                collective_id=0, has_side_effects=True, vmem_limit_bytes=60 * 1024 * 1024,
            ),
        )(attn_out, w_blocks, w_scales, residual)
        normed = (hidden.astype(f32) * gain[None, :] * scale[:, :1]).astype(bf16)
        return hidden, normed

    return jax.shard_map(
        on_device,
        mesh=mesh,
        in_specs=(
            P("dp", "tensor"),
            P("tensor", "dp"),
            P("tensor", "dp"),
            P("dp", None),
            P("tensor"),
        ),
        out_specs=(P("dp", "tensor"), P("dp", "tensor")),
        check_vma=False,
    )
```
